32 devices in a mesh: member: 4 (over y, x), region: 2 (over core), block: 4 (over z).
Axes of the slice: x: 2, y: 2, z: 4, core: 2. Of those that a mesh axis runs over, the one named last changes fastest.
Arguments:
- traffic_load: float32 [128, 65536], P('member', ('region', 'block')), may hold values from 0.05 to 0.7
- free_speed: float32 [65536], P(('region', 'block')), may hold values from 0.3 to 0.95
- wave_speed: float32 [65536], P(('region', 'block')), may hold values from 0.15 to 0.6
- jam_density: float32 [65536], P(('region', 'block')), may hold values from 0.8 to 1.2
- capacity_share: float32 [65536], P(('region', 'block')), may hold values from 0.5 to 1
- observation_cell: int32 [24576], P(('region', 'block')), may hold values from 0 to 2047
- obs_count: int32 [32], P(('region', 'block')), may hold values from 1 to 768, 12288 in all
- observation_value: float32 [24576], P(('region', 'block')), may hold values from 0 to 0.8
- observation_variance: float32 [24576], P(('region', 'block')), may hold values from 0.002 to 0.02
- observation_noise: float32 [128, 24576], P('member', ('region', 'block')), may hold values from -6 to 6
- block_lists: int32 [32, 3], P(('region', 'block')), may hold values from 0 to 31, as said below
Outputs:
- analysis: float32 [128, 65536], P('member', ('region', 'block'))
The draws below stay inside these ranges and needn't reach their ends.
Inputs may be any that keep to these rules, and one draw needn't show every extreme that they name: `block_lists`: row b lists 3 different blocks, b itself among them, each within 4 blocks of b.
All inputs are finite; a program needn't handle non-finite values. No bound on the sum of `obs_count` on one device may be relied on, other than what follows from the above.
Results may differ from the reference program's by a relative error of at most 0.0003.
Values sent between devices are 32-bit elements; how exact they have to be, the bound alone decides.
A program may use at most 64 MiB of HBM per device.

```python
import math
import jax
import jax.numpy as jnp
import numpy as np
from jax import lax

REALIZATION_TALLY = 128
HORIZON_TICKS = 16
BLK_DEV = 4
NEIGH = 3
CELLS_PER_BLOCK = 2048
BLOCK_SLOTS = 768
NBLK = 32
NC = 65536
SLOT_COUNT = 24576


def draw_block_lists(key, part):
    reach_blocks = BLK_DEV
    span_count = 2 * reach_blocks + 1
    offsets = jnp.arange(span_count, dtype=jnp.int32) - reach_blocks
    owner_block = jnp.arange(NBLK, dtype=jnp.int32)[:, None]
    candidate = owner_block + offsets[None, :]
    usable = (candidate >= 0) & (candidate < NBLK)
    ranking = jax.random.randint(jax.random.fold_in(key, 17), (NBLK, span_count), 0, 1000, dtype=jnp.int32) * span_count + jnp.arange(span_count, dtype=jnp.int32)[None, :]
    ranking = jnp.where(usable, ranking, -1 - jnp.arange(span_count, dtype=jnp.int32)[None, :])
    ranking = jnp.where(offsets[None, :] == 0, 2000 * span_count, ranking)
    scores_top, chosen = lax.top_k(ranking, NEIGH)
    return jnp.take_along_axis(candidate, chosen, axis=1).astype(jnp.int32)


def set_ends(array, rng, low, top_value):
    extent = array.shape
    index_at = [jax.random.randint(jax.random.fold_in(rng, axis), (), 0, extent[axis]) for axis in range(len(extent))]
    array = array.at[tuple(index_at)].set(low)
    longest = extent.index(max(extent))
    index_at[longest] = (index_at[longest] + 1) % extent[longest]
    return array.at[tuple(index_at)].set(top_value)


def shard_levels(key, dims, shards, least, largest):
    level, own = 1.0, jax.random.fold_in(key, 6)
    for position, shards_of in shards:
        heights = jnp.exp(jax.random.uniform(jax.random.fold_in(own, position), (shards_of,), jnp.float32, least / len(shards), largest / len(shards)))
        level = level * jnp.repeat(heights, dims[position] // shards_of).reshape([-1 if axis == position else 1 for axis in range(len(dims))])
    return level


def split_up(number_of, total, most, skew):
    portions = [(1 << 20) // math.isqrt(standing ** skew) + 1 for standing in range(2, number_of + 1)]
    rest, given = total - most - (number_of - 1), [1] * (number_of - 1)
    while rest > 0:
        candidates = [i for i in range(number_of - 1) if given[i] < most]
        mass, budget = sum([portions[i] for i in candidates]), rest
        for i in candidates:
            addition = min(most - given[i], max(1, budget * portions[i] // mass), rest)
            given[i] = given[i] + addition
            rest = rest - addition
    return np.array([most] + given)


def ragged_sizes(key, number_of, total, bound, lean):
    if number_of == 2:
        one = jax.random.randint(key, (), max(1, total - bound), min(bound, total - 1) + 1)
        return jnp.stack([one, total - one])
    sizes = jnp.asarray(split_up(number_of, total, bound, lean), jnp.int32)
    couples = (number_of - 1) // 2
    donor, taker = sizes[1:1 + 2 * couples:2], sizes[2:2 + 2 * couples:2]
    room = jnp.minimum(donor - 1, bound - taker)
    shifted = jax.random.randint(jax.random.fold_in(key, 1), (couples,), 0, 1 << 20) % (room + 1)
    sizes = sizes.at[1:1 + 2 * couples:2].set(donor - shifted).at[2:2 + 2 * couples:2].set(taker + shifted)
    return sizes[jax.random.permutation(jax.random.fold_in(key, 2), number_of)]


def normal_values(stream_key, dims, width, most, cuts=(), kind=jnp.bfloat16):
    entries = width * jax.random.normal(stream_key, dims, jnp.float32)
    if cuts:
        entries = entries * shard_levels(stream_key, dims, cuts, -0.22, 0.18)
    return jnp.clip(entries, -most, most).astype(kind)


def setup_inputs(seed: int = 0) -> dict:
    seeds = jax.random.split(jax.random.key(seed), 12)
    return {
        "traffic_load": jnp.clip(0.05 + 0.65 * jax.random.uniform(seeds[0], (REALIZATION_TALLY, NC), jnp.float32) ** shard_levels(seeds[0], (REALIZATION_TALLY, NC), ((0, 4), (1, 8)), -0.2, 0.2), 0.05, 0.7),
        "free_speed": jnp.clip(jnp.exp(math.log(0.95) - 1.1526795 * jax.random.uniform(seeds[1], (NC,), jnp.float32) ** shard_levels(seeds[1], (NC,), ((0, 8),), -0.2, 0.2)), 0.3, 0.95),
        "wave_speed": jnp.clip(jnp.exp(math.log(0.6) - 1.3862944 * jax.random.uniform(seeds[2], (NC,), jnp.float32) ** shard_levels(seeds[2], (NC,), ((0, 8),), -0.2, 0.2)), 0.15, 0.6),
        "jam_density": jnp.clip(0.8 + 0.40000004 * jax.random.uniform(seeds[3], (NC,), jnp.float32) ** shard_levels(seeds[3], (NC,), ((0, 8),), -0.2, 0.2), 0.8, 1.2),
        "capacity_share": jnp.clip(0.5 + 0.5 * jax.random.uniform(seeds[4], (NC,), jnp.float32) ** shard_levels(seeds[4], (NC,), ((0, 8),), -0.2, 0.2), 0.5, 1.0),
        "observation_cell": set_ends(jax.random.randint(seeds[5], (SLOT_COUNT,), 0, CELLS_PER_BLOCK), jax.random.fold_in(seeds[5], 1), 0, CELLS_PER_BLOCK - 1).astype(jnp.int32),
        "obs_count": ragged_sizes(seeds[6], NBLK, NBLK * BLOCK_SLOTS // 2, BLOCK_SLOTS, 2).astype(jnp.int32),
        "observation_value": jnp.clip(0.8 * jax.random.uniform(seeds[7], (SLOT_COUNT,), jnp.float32) ** shard_levels(seeds[7], (SLOT_COUNT,), ((0, 8),), -0.2, 0.2), 0.0, 0.8),
        "observation_variance": jnp.clip(jnp.exp(math.log(0.02) - 2.30258502 * jax.random.uniform(seeds[8], (SLOT_COUNT,), jnp.float32) ** shard_levels(seeds[8], (SLOT_COUNT,), ((0, 8),), -0.2, 0.2)), 0.002, 0.02),
        "observation_noise": normal_values(seeds[9], (REALIZATION_TALLY, SLOT_COUNT), 1.0, 6.0, ((0, 4), (1, 8)), jnp.float32),
        "block_lists": draw_block_lists(jax.random.fold_in(seeds[11], 71), 0),
    }


def road_capacity(free_speed, wave_speed, jam_density, capacity_share):
    return capacity_share * free_speed * wave_speed * jam_density / (free_speed + wave_speed)

def block_products(left_side, right_side, weight, block_total):
    member_count = left_side.shape[0]
    left_blocks = (left_side * weight).reshape(member_count, block_total, -1)
    right_blocks = right_side.reshape(member_count, block_total, -1)
    return jnp.einsum('kbo,jbo->bkj', left_blocks, right_blocks, precision=lax.Precision.HIGHEST)

def reference(traffic_load, free_speed, wave_speed, jam_density, capacity_share, observation_cell, obs_count, observation_value, observation_variance, observation_noise, block_lists):
    capacity = road_capacity(free_speed, wave_speed, jam_density, capacity_share)
    member_count = traffic_load.shape[0]

    def propagate_traffic_load(step_index, state):
        demand = jnp.minimum(free_speed * state, capacity)
        supply = jnp.minimum(capacity, wave_speed * (jam_density - state))
        upstream = jnp.concatenate([jnp.zeros((member_count, 1), demand.dtype), demand], axis=1)
        exit_column = jnp.broadcast_to(capacity[-1:][None, :], (member_count, 1)).astype(supply.dtype)
        downstream = jnp.concatenate([supply, exit_column], axis=1)
        fluxes = jnp.minimum(upstream, downstream)
        return state + fluxes[:, :-1] - fluxes[:, 1:]
    predicted_traffic_load = lax.fori_loop(0, HORIZON_TICKS, propagate_traffic_load, traffic_load)
    realization_average = lax.optimization_barrier(jnp.sum(predicted_traffic_load, axis=0)) / REALIZATION_TALLY
    realization_departure = predicted_traffic_load - realization_average
    slot_cell_index = jnp.arange(SLOT_COUNT, dtype=jnp.int32) // BLOCK_SLOTS * CELLS_PER_BLOCK + observation_cell.astype(jnp.int32)
    obs_anomaly = jnp.take(realization_departure, slot_cell_index, axis=1)
    obs_mean = jnp.take(realization_average, slot_cell_index)
    live_mask = (jnp.arange(BLOCK_SLOTS, dtype=jnp.int32)[None, :] < obs_count[:, None]).reshape(-1).astype(observation_variance.dtype)
    weight = live_mask / observation_variance
    misfit = observation_value - obs_mean
    spread = lax.optimization_barrier(jnp.sum(obs_anomaly * obs_anomaly, axis=0)) / (REALIZATION_TALLY - 1)
    misfit_sum = jnp.sum(misfit * misfit * weight)
    spread_sum = jnp.sum(live_mask * (spread / observation_variance + 1.0))
    inflation = jnp.sqrt(misfit_sum / spread_sum)
    perturbed = misfit + jnp.sqrt(observation_variance) * observation_noise
    gram_part = block_products(obs_anomaly, obs_anomaly, weight, NBLK)
    cross_part = block_products(obs_anomaly, perturbed, weight, NBLK)
    local_gram = gram_part[block_lists[:, 0]]
    local_cross = cross_part[block_lists[:, 0]]
    for entry in range(1, NEIGH):
        local_gram = local_gram + gram_part[block_lists[:, entry]]
        local_cross = local_cross + cross_part[block_lists[:, entry]]
    system = (REALIZATION_TALLY - 1) * jnp.eye(REALIZATION_TALLY, dtype=local_gram.dtype)[None] + inflation * inflation * local_gram
    right_side = inflation * local_cross - inflation * inflation * local_gram
    mixing = jnp.linalg.solve(system, right_side)
    anomaly_blocks = realization_departure.reshape(member_count, NBLK, CELLS_PER_BLOCK)
    change = jnp.einsum('kbc,bkj->jbc', anomaly_blocks, mixing, precision=lax.Precision.HIGHEST).reshape(member_count, NC)
    return realization_average + inflation * realization_departure + inflation * change
```

```python
import functools

import jax
import jax.numpy as jnp
from jax import lax
from jax.experimental import pallas as pl
from jax.experimental.pallas import tpu as pltpu
from jax.sharding import PartitionSpec as P

HORIZON_TICKS = 16
HALO = 128
HIGHEST = lax.Precision.HIGHEST
MESH = pl.DeviceIdType.MESH
VMEM = pl.BlockSpec(memory_space=pltpu.VMEM)
SMEM = pl.BlockSpec(memory_space=pltpu.SMEM)


def position(regions, blocks):
    slab = lax.axis_index("region") * blocks + lax.axis_index("block")
    return lax.axis_index("member"), slab


def device(member, slab, blocks):
    return {"member": member, "region": lax.div(slab, blocks), "block": lax.rem(slab, blocks)}


def remote(src, dst, send_sem, recv_sem, target):
    return pltpu.make_async_remote_copy(
        src_ref=src,
        dst_ref=dst,
        send_sem=send_sem,
        recv_sem=recv_sem,
        device_id=target,
        device_id_type=MESH,
    )


def greet(target):
    pl.semaphore_signal(
        pltpu.get_barrier_semaphore(), inc=1, device_id=target, device_id_type=MESH
    )


def scatter_kernel(
    sizes,
    load,
    noise,
    road,
    state,
    noise_all,
    road_all,
    main_send,
    main_recv,
    left_send,
    left_recv,
    right_send,
    right_recv,
    noise_send,
    noise_recv,
    edge_send,
    road_send,
    road_recv,
):
    members, regions, blocks = sizes
    slabs = regions * blocks
    me, slab = position(regions, blocks)
    rows = load.shape[0]
    cells = load.shape[1] // members
    slots = noise.shape[1] // members
    has_left, has_right = slab > 0, slab < slabs - 1
    first, last = me == 0, me == members - 1

    for r in range(1, members):
        greet(device(lax.rem(me + r, members), slab, blocks))

    @pl.when(first & has_left)
    def _():
        for other in range(members):
            greet(device(other, slab - 1, blocks))

    @pl.when(last & has_right)
    def _():
        for other in range(members):
            greet(device(other, slab + 1, blocks))

    pl.semaphore_wait(
        pltpu.get_barrier_semaphore(),
        members - 1 + has_left.astype(jnp.int32) + has_right.astype(jnp.int32),
    )

    mine = pl.ds(pl.multiple_of(me * rows, rows), rows)
    centre = pl.ds(HALO, cells)
    left = pl.ds(0, HALO)
    right = pl.ds(HALO + cells, HALO)

    def own(start, size):
        return pl.ds(pl.multiple_of(start, HALO), size)

    def edge_right():
        return remote(
            load.at[:, members * cells - HALO :],
            state.at[mine, left],
            edge_send.at[0],
            left_recv.at[me],
            device(0, slab + 1, blocks),
        )

    def edge_left():
        return remote(
            load.at[:, :HALO],
            state.at[mine, right],
            edge_send.at[1],
            right_recv.at[me],
            device(members - 1, slab - 1, blocks),
        )

    def road_right():
        return remote(
            road.at[:, members * cells - HALO :],
            road_all.at[:, left],
            road_send.at[0],
            road_recv.at[0],
            device(0, slab + 1, blocks),
        )

    def road_left():
        return remote(
            road.at[:, :HALO],
            road_all.at[:, right],
            road_send.at[1],
            road_recv.at[1],
            device(members - 1, slab - 1, blocks),
        )

    def main_copy(r):
        to = lax.rem(me + r, members)
        return remote(
            load.at[:, own(to * cells, cells)],
            state.at[mine, centre],
            main_send.at[r - 1],
            main_recv.at[me],
            device(to, slab, blocks),
        )

    def left_copy(r):
        to = lax.rem(me + r, members)
        return to > 0, remote(
            load.at[:, own(jnp.maximum(to * cells - HALO, 0), HALO)],
            state.at[mine, left],
            left_send.at[r - 1],
            left_recv.at[me],
            device(to, slab, blocks),
        )

    def right_copy(r):
        to = lax.rem(me + r, members)
        return to < members - 1, remote(
            load.at[:, own(jnp.minimum((to + 1) * cells, (members - 1) * cells), HALO)],
            state.at[mine, right],
            right_send.at[r - 1],
            right_recv.at[me],
            device(to, slab, blocks),
        )

    def noise_copy(r):
        to = lax.rem(me + r, members)
        return remote(
            noise.at[:, own(to * slots, slots)],
            noise_all.at[mine, :],
            noise_send.at[r - 1],
            noise_recv.at[me],
            device(to, slab, blocks),
        )

    @pl.when(has_right)
    def _():
        edge_right().start()

    @pl.when(has_left)
    def _():
        edge_left().start()

    @pl.when(has_right & first)
    def _():
        road_right().start()

    @pl.when(has_left & last)
    def _():
        road_left().start()

    for r in range(1, members):
        for needed, copy in (left_copy(r), right_copy(r)):
            pl.when(needed)(copy.start)
    for r in range(1, members):
        main_copy(r).start()
    for r in range(1, members):
        noise_copy(r).start()

    state[mine, centre] = load[:, own(me * cells, cells)]
    noise_all[mine, :] = noise[:, own(me * slots, slots)]
    road_all[:, centre] = road[:, own(me * cells, cells)]

    @pl.when(jnp.logical_not(first))
    def _():
        spot = own(jnp.maximum(me * cells - HALO, 0), HALO)
        state[mine, left] = load[:, spot]
        road_all[:, left] = road[:, spot]

    @pl.when(jnp.logical_not(last))
    def _():
        spot = own(jnp.minimum((me + 1) * cells, (members - 1) * cells), HALO)
        state[mine, right] = load[:, spot]
        road_all[:, right] = road[:, spot]

    @pl.when(first & jnp.logical_not(has_left))
    def _():
        state[:, left] = jnp.zeros((members * rows, HALO), jnp.float32)
        road_all[:, left] = jnp.zeros((8, HALO), jnp.float32)

    @pl.when(last & jnp.logical_not(has_right))
    def _():
        state[:, right] = jnp.zeros((members * rows, HALO), jnp.float32)
        row = lax.broadcasted_iota(jnp.int32, (8, HALO), 0)
        exit_value = road[:, members * cells - 1 :]
        ghost = jnp.where(row == 1, 1.0, jnp.where(row == 2, 1e30, 0.0))
        road_all[:, right] = jnp.where(row == 3, exit_value, ghost)

    def arrive(dst, sem):
        remote(dst, dst, main_send.at[0], sem, device(lax.rem(me + 1, members), slab, blocks)).wait_recv()

    for r in range(1, members):
        origin = lax.rem(me + r, members)
        from_rows = pl.ds(pl.multiple_of(origin * rows, rows), rows)
        arrive(state.at[from_rows, centre], main_recv.at[origin])
        arrive(noise_all.at[from_rows, :], noise_recv.at[origin])

        @pl.when(jnp.logical_not(first))
        def _():
            arrive(state.at[from_rows, left], left_recv.at[origin])

        @pl.when(jnp.logical_not(last))
        def _():
            arrive(state.at[from_rows, right], right_recv.at[origin])

    @pl.when(first & has_left)
    def _():
        for origin in range(members):
            arrive(state.at[pl.ds(origin * rows, rows), left], left_recv.at[origin])
        arrive(road_all.at[:, left], road_recv.at[0])

    @pl.when(last & has_right)
    def _():
        for origin in range(members):
            arrive(state.at[pl.ds(origin * rows, rows), right], right_recv.at[origin])
        arrive(road_all.at[:, right], road_recv.at[1])

    for r in range(1, members):
        main_copy(r).wait_send()
        noise_copy(r).wait_send()
        for needed, copy in (left_copy(r), right_copy(r)):
            pl.when(needed)(copy.wait_send)

    @pl.when(has_right)
    def _():
        edge_right().wait_send()

    @pl.when(has_left)
    def _():
        edge_left().wait_send()

    @pl.when(has_right & first)
    def _():
        road_right().wait_send()

    @pl.when(has_left & last)
    def _():
        road_left().wait_send()


def block_kernel(
    sizes, counts, state, noise, road, cell, value, variance, anomaly, mean, products, parts, roads, forecast
):
    members, regions, blocks = sizes
    me = lax.axis_index("member")
    rows, width = state.shape
    cells = width - 2 * HALO
    slots = noise.shape[1]
    for i in range(4):
        roads[i] = jnp.broadcast_to(road[i : i + 1, :], (8, width))

    step_rows = 8

    def group(g, total):
        here = pl.ds(pl.multiple_of(g * step_rows, step_rows), step_rows)

        def tick(_, now):
            cap = roads[3]
            demand = jnp.minimum(roads[0] * now, cap)
            supply = jnp.minimum(cap, roads[1] * (roads[2] - now))
            flux = jnp.minimum(demand, pltpu.roll(supply, width - 1, 1))
            return now + pltpu.roll(flux, 1, 1) - flux

        done = lax.fori_loop(0, HORIZON_TICKS, tick, state[here, :])
        inner = done[:, HALO : HALO + cells]
        forecast[here, :] = inner
        return total + inner

    total = lax.fori_loop(0, rows // step_rows, group, jnp.zeros((step_rows, cells), jnp.float32))
    average = jnp.sum(total, axis=0, keepdims=True) / rows
    mean[...] = jnp.broadcast_to(average, mean.shape)

    mine = pl.ds(pl.multiple_of(me * slots, HALO), slots)
    spots = cell[:, mine]
    depth = 256
    picked = jnp.zeros((3 * rows, slots), jnp.float32)
    for c in range(cells // depth):
        part = forecast[:, c * depth : (c + 1) * depth]
        high = part.astype(jnp.bfloat16)
        rest = part - high.astype(jnp.float32)
        middle = rest.astype(jnp.bfloat16)
        low = (rest - middle.astype(jnp.float32)).astype(jnp.bfloat16)
        hot = lax.broadcasted_iota(jnp.int32, (depth, slots), 0) + c * depth == spots
        picked = picked + jnp.dot(
            jnp.concatenate([high, middle, low], axis=0),
            jnp.where(hot, 1.0, 0.0).astype(jnp.bfloat16),
            preferred_element_type=jnp.float32,
        )
        anomaly[:, c * depth : (c + 1) * depth] = part - average[:, c * depth : (c + 1) * depth]
    seen = picked[:rows] + picked[rows : 2 * rows] + picked[2 * rows :]
    obs_mean = jnp.sum(seen, axis=0, keepdims=True) / rows
    departure = seen - obs_mean
    var = variance[:, mine]
    live = (lax.broadcasted_iota(jnp.int32, (1, slots), 1) < counts[me]).astype(jnp.float32)
    weight = live / var
    misfit = value[:, mine] - obs_mean
    spread = jnp.sum(departure * departure, axis=0, keepdims=True) / (rows - 1)
    first = jnp.sum(misfit * misfit * weight, axis=1, keepdims=True)
    second = jnp.sum(live * (spread / var + 1.0), axis=1, keepdims=True)
    row = lax.broadcasted_iota(jnp.int32, parts.shape, 0)
    parts[...] = jnp.where(row == 0, first, jnp.where(row == 1, second, 0.0))
    scaled = departure * weight
    perturbed = misfit + jnp.sqrt(var) * noise[...]
    contract = (((1,), (1,)), ((), ()))
    products[:, :rows] = lax.dot_general(
        scaled, departure, contract, precision=HIGHEST, preferred_element_type=jnp.float32
    )
    products[:, rows:] = lax.dot_general(
        scaled, perturbed, contract, precision=HIGHEST, preferred_element_type=jnp.float32
    )


def neighbour_kernel(
    sizes,
    select,
    products,
    parts,
    total,
    sums,
    slab_in,
    outgoing,
    incoming,
    parts_in,
    parts_sum,
    parts_all,
    slab_send,
    slab_recv,
    plane_send,
    plane_recv,
    part_send,
    part_recv,
    wide_send,
    wide_recv,
):
    members, regions, blocks = sizes
    slabs = regions * blocks
    me, slab = position(regions, blocks)
    has_left, has_right = slab > 0, slab < slabs - 1
    for r in range(1, members):
        greet(device(lax.rem(me + r, members), slab, blocks))
    for r in range(1, slabs):
        greet(device(me, lax.rem(slab + r, slabs), blocks))
    pl.semaphore_wait(pltpu.get_barrier_semaphore(), members + slabs - 2)

    def up():
        return remote(
            products, slab_in.at[0], slab_send.at[0], slab_recv.at[0], device(me, slab + 1, blocks)
        )

    def down():
        return remote(
            products, slab_in.at[1], slab_send.at[1], slab_recv.at[1], device(me, slab - 1, blocks)
        )

    def part_copy(r):
        to = lax.rem(me + r, members)
        return remote(
            parts, parts_in.at[me], part_send.at[r - 1], part_recv.at[me], device(to, slab, blocks)
        )

    def wide_copy(r):
        to = lax.rem(slab + r, slabs)
        return remote(
            parts_sum, parts_all.at[slab], wide_send.at[r - 1], wide_recv.at[slab], device(me, to, blocks)
        )

    def plane_copy(r):
        to = lax.rem(me + r, members)
        return remote(
            outgoing.at[r - 1],
            incoming.at[r - 1],
            plane_send.at[r - 1],
            plane_recv.at[r - 1],
            device(to, slab, blocks),
        )

    for r in range(1, members):
        part_copy(r).start()

    @pl.when(has_right)
    def _():
        up().start()

    @pl.when(has_left)
    def _():
        down().start()

    gathered = parts[...]
    for r in range(1, members):
        origin = lax.rem(me + r, members)
        remote(
            parts, parts_in.at[origin], part_send.at[0], part_recv.at[origin], device(origin, slab, blocks)
        ).wait_recv()
        gathered = gathered + parts_in[origin]
    parts_sum[...] = gathered
    for r in range(1, slabs):
        wide_copy(r).start()

    @pl.when(has_left)
    def _():
        up().wait_recv()

    @pl.when(jnp.logical_not(has_left))
    def _():
        slab_in[0] = jnp.zeros_like(slab_in[0])

    @pl.when(has_right)
    def _():
        down().wait_recv()

    @pl.when(jnp.logical_not(has_right))
    def _():
        slab_in[1] = jnp.zeros_like(slab_in[1])

    def blend(to):
        return (
            select[to * 3] * slab_in[0]
            + select[to * 3 + 1] * products[...]
            + select[to * 3 + 2] * slab_in[1]
        )

    for r in range(1, members):
        outgoing[r - 1] = blend(lax.rem(me + r, members))
        plane_copy(r).start()
    local = blend(me)

    for r in range(1, slabs):
        origin = lax.rem(slab + r, slabs)
        remote(
            parts_sum, parts_all.at[origin], wide_send.at[0], wide_recv.at[origin], device(me, origin, blocks)
        ).wait_recv()
        gathered = gathered + parts_all[origin]
    sums[...] = gathered

    for r in range(1, members):
        plane_copy(r).wait_recv()
        local = local + incoming[r - 1]
    total[...] = local

    for r in range(1, members):
        part_copy(r).wait_send()
        plane_copy(r).wait_send()
    for r in range(1, slabs):
        wide_copy(r).wait_send()

    @pl.when(has_right)
    def _():
        up().wait_send()

    @pl.when(has_left)
    def _():
        down().wait_send()


def dot(a, b):
    return jnp.dot(a, b, precision=HIGHEST, preferred_element_type=jnp.float32)


def invert(block):
    size = block.shape[0]
    row = lax.broadcasted_iota(jnp.int32, (size, size), 0)
    column = lax.broadcasted_iota(jnp.int32, (size, size), 1)
    work = block
    for k in range(size):
        scale = 1.0 / work[k : k + 1, k : k + 1]
        pivot = jnp.where(column[k : k + 1] == k, 1.0, work[k : k + 1, :]) * scale
        factor = work[:, k : k + 1]
        work = jnp.where(
            row == k, pivot, jnp.where(column == k, 0.0, work) - factor * pivot
        )
    return work


def solve_kernel(sizes, total, sums, anomaly, mean, result, work):
    rows = total.shape[0]
    size = 16
    inflation = jnp.sqrt(sums[0:1, 0:1] / sums[1:2, 0:1])
    diagonal = (
        lax.broadcasted_iota(jnp.int32, (rows, rows), 0)
        == lax.broadcasted_iota(jnp.int32, (rows, rows), 1)
    )
    identity = jnp.where(diagonal, float(rows - 1), 0.0)
    work[:, :rows] = identity + inflation * inflation * total[:, :rows]
    work[:, rows:] = identity + inflation * total[:, rows:]
    for p in range(rows // size):
        top, end = p * size, (p + 1) * size
        panel = work[top:end, :]
        update = dot(invert(panel[:, top:end]), panel)
        factor = work[:, top:end]
        work[...] = work[...] - dot(factor, update)
        work[top:end, :] = update
    mixing = inflation * work[:, rows:]
    result[...] = mean[0:1, :] + lax.dot_general(
        mixing,
        anomaly[...],
        (((0,), (0,)), ((), ())),
        precision=HIGHEST,
        preferred_element_type=jnp.float32,
    )


def return_kernel(sizes, result, analysis, send, recv):
    members, regions, blocks = sizes
    me, slab = position(regions, blocks)
    rows = analysis.shape[0]
    cells = result.shape[1]
    for r in range(1, members):
        greet(device(lax.rem(me + r, members), slab, blocks))
    pl.semaphore_wait(pltpu.get_barrier_semaphore(), members - 1)

    def copy(r):
        to = lax.rem(me + r, members)
        return remote(
            result.at[pl.ds(pl.multiple_of(to * rows, rows), rows), :],
            analysis.at[:, pl.ds(pl.multiple_of(me * cells, HALO), cells)],
            send.at[r - 1],
            recv.at[me],
            device(to, slab, blocks),
        )

    for r in range(1, members):
        copy(r).start()
    analysis[:, pl.ds(pl.multiple_of(me * cells, HALO), cells)] = result[
        pl.ds(pl.multiple_of(me * rows, rows), rows), :
    ]
    for r in range(1, members):
        origin = lax.rem(me + r, members)
        spot = analysis.at[:, pl.ds(pl.multiple_of(origin * cells, HALO), cells)]
        remote(spot, spot, send.at[0], recv.at[origin], device(origin, slab, blocks)).wait_recv()
    for r in range(1, members):
        copy(r).wait_send()


def body(
    sizes,
    traffic_load,
    free_speed,
    wave_speed,
    jam_density,
    capacity_share,
    observation_cell,
    obs_count,
    observation_value,
    observation_variance,
    observation_noise,
    block_lists,
):
    members, regions, blocks = sizes
    slabs = regions * blocks
    mem_local, cell_total = traffic_load.shape
    slot_total = observation_cell.shape[0]
    block_total = obs_count.shape[0]
    assert block_total == members
    rows, cells, slots = mem_local * members, cell_total // members, slot_total // members
    f32 = jnp.float32
    dma = pltpu.SemaphoreType.DMA

    capacity = capacity_share * free_speed * wave_speed * jam_density / (free_speed + wave_speed)
    blank = jnp.zeros_like(capacity)
    road = jnp.stack([free_speed, wave_speed, jam_density, capacity, blank, blank, blank, blank])

    state, noise_all, road_all = pl.pallas_call(
        functools.partial(scatter_kernel, sizes),
        out_shape=(
            jax.ShapeDtypeStruct((rows, cells + 2 * HALO), f32),
            jax.ShapeDtypeStruct((rows, slots), f32),
            jax.ShapeDtypeStruct((8, cells + 2 * HALO), f32),
        ),
        in_specs=[VMEM] * 3,
        out_specs=(VMEM,) * 3,
        scratch_shapes=[
            dma((members - 1,)),
            dma((members,)),
            dma((members - 1,)),
            dma((members,)),
            dma((members - 1,)),
            dma((members,)),
            dma((members - 1,)),
            dma((members,)),
            dma((2,)),
            dma((2,)),
            dma((2,)),
        ],
        compiler_params=pltpu.CompilerParams(collective_id=0, has_side_effects=True),
        name="scatter",
    )(traffic_load, observation_noise, road)

    anomaly, mean, products, parts = pl.pallas_call(
        functools.partial(block_kernel, sizes),
        out_shape=(
            jax.ShapeDtypeStruct((rows, cells), f32),
            jax.ShapeDtypeStruct((8, cells), f32),
            jax.ShapeDtypeStruct((rows, 2 * rows), f32),
            jax.ShapeDtypeStruct((8, HALO), f32),
        ),
        in_specs=[SMEM] + [VMEM] * 6,
        out_specs=(VMEM,) * 4,
        scratch_shapes=[
            pltpu.VMEM((4, 8, cells + 2 * HALO), f32),
            pltpu.VMEM((rows, cells), f32),
        ],
        name="block",
    )(
        obs_count,
        state,
        noise_all,
        road_all,
        observation_cell.reshape(1, -1),
        observation_value.reshape(1, -1),
        observation_variance.reshape(1, -1),
    )

    slab = lax.axis_index(("region", "block"))
    named = (slab + jnp.arange(-1, 2, dtype=jnp.int32)) * block_total + lax.axis_index("member")
    select = jnp.sum((block_lists[:, None, :] == named[None, :, None]).astype(f32), axis=2).reshape(-1)

    total, sums = pl.pallas_call(
        functools.partial(neighbour_kernel, sizes),
        out_shape=(
            jax.ShapeDtypeStruct((rows, 2 * rows), f32),
            jax.ShapeDtypeStruct((8, HALO), f32),
        ),
        in_specs=[SMEM, VMEM, VMEM],
        out_specs=(VMEM, VMEM),
        scratch_shapes=[
            pltpu.VMEM((2, rows, 2 * rows), f32),
            pltpu.VMEM((members - 1, rows, 2 * rows), f32),
            pltpu.VMEM((members - 1, rows, 2 * rows), f32),
            pltpu.VMEM((members, 8, HALO), f32),
            pltpu.VMEM((8, HALO), f32),
            pltpu.VMEM((slabs, 8, HALO), f32),
            dma((2,)),
            dma((2,)),
            dma((members - 1,)),
            dma((members - 1,)),
            dma((members - 1,)),
            dma((members,)),
            dma((slabs - 1,)),
            dma((slabs,)),
        ],
        compiler_params=pltpu.CompilerParams(collective_id=1, has_side_effects=True),
        name="neighbours",
    )(select, products, parts)

    result = pl.pallas_call(
        functools.partial(solve_kernel, sizes),
        out_shape=jax.ShapeDtypeStruct((rows, cells), f32),
        in_specs=[VMEM] * 4,
        out_specs=VMEM,
        scratch_shapes=[pltpu.VMEM((rows, 2 * rows), f32)],
        name="solve",
    )(total, sums, anomaly, mean)

    return pl.pallas_call(
        functools.partial(return_kernel, sizes),
        out_shape=jax.ShapeDtypeStruct((mem_local, cell_total), f32),
        in_specs=[VMEM],
        out_specs=VMEM,
        scratch_shapes=[dma((members - 1,)), dma((members,))],
        compiler_params=pltpu.CompilerParams(collective_id=2, has_side_effects=True),
        name="give_back",
    )(result)


def solution(mesh):
    slab = P(("region", "block"))
    placed = (
        P("member", ("region", "block")),
        slab,
        slab,
        slab,
        slab,
        slab,
        slab,
        slab,
        slab,
        P("member", ("region", "block")),
        P(("region", "block"), None),
    )
    sizes = (mesh.shape["member"], mesh.shape["region"], mesh.shape["block"])
    return jax.shard_map(
        functools.partial(body, sizes),
        mesh=mesh,
        in_specs=placed,
        out_specs=P("member", ("region", "block")),
        check_vma=False,
    )
```

```python
import functools

import jax
import jax.numpy as jnp
from jax import lax
from jax.experimental import pallas as pl
from jax.experimental.pallas import tpu as pltpu
from jax.sharding import PartitionSpec as P

HORIZON_TICKS = 16
HALO = 128
HIGHEST = lax.Precision.HIGHEST
MESH = pl.DeviceIdType.MESH
VMEM = pl.BlockSpec(memory_space=pltpu.VMEM)
SMEM = pl.BlockSpec(memory_space=pltpu.SMEM)


def position(regions, blocks):
    slab = lax.axis_index("region") * blocks + lax.axis_index("block")
    return lax.axis_index("member"), slab


def device(member, slab, blocks):
    return {"member": member, "region": lax.div(slab, blocks), "block": lax.rem(slab, blocks)}


def remote(src, dst, send_sem, recv_sem, target):
    return pltpu.make_async_remote_copy(
        src_ref=src,
        dst_ref=dst,
        send_sem=send_sem,
        recv_sem=recv_sem,
        device_id=target,
        device_id_type=MESH,
    )


def greet(target):
    pl.semaphore_signal(
        pltpu.get_barrier_semaphore(), inc=1, device_id=target, device_id_type=MESH
    )


def scatter_kernel(
    sizes,
    load,
    noise,
    road,
    state,
    noise_all,
    road_all,
    main_send,
    main_recv,
    left_send,
    left_recv,
    right_send,
    right_recv,
    noise_send,
    noise_recv,
    edge_send,
    road_send,
    road_recv,
):
    members, regions, blocks = sizes
    slabs = regions * blocks
    me, slab = position(regions, blocks)
    rows = load.shape[0]
    cells = load.shape[1] // members
    slots = noise.shape[1] // members
    has_left, has_right = slab > 0, slab < slabs - 1
    first, last = me == 0, me == members - 1

    for r in range(1, members):
        greet(device(lax.rem(me + r, members), slab, blocks))

    @pl.when(first & has_left)
    def _():
        for other in range(members):
            greet(device(other, slab - 1, blocks))

    @pl.when(last & has_right)
    def _():
        for other in range(members):
            greet(device(other, slab + 1, blocks))

    pl.semaphore_wait(
        pltpu.get_barrier_semaphore(),
        members - 1 + has_left.astype(jnp.int32) + has_right.astype(jnp.int32),
    )

    mine = pl.ds(pl.multiple_of(me * rows, rows), rows)
    centre = pl.ds(HALO, cells)
    left = pl.ds(0, HALO)
    right = pl.ds(HALO + cells, HALO)

    def own(start, size):
        return pl.ds(pl.multiple_of(start, HALO), size)

    def edge_right():
        return remote(
            load.at[:, members * cells - HALO :],
            state.at[mine, left],
            edge_send.at[0],
            left_recv.at[me],
            device(0, slab + 1, blocks),
        )

    def edge_left():
        return remote(
            load.at[:, :HALO],
            state.at[mine, right],
            edge_send.at[1],
            right_recv.at[me],
            device(members - 1, slab - 1, blocks),
        )

    def road_right():
        return remote(
            road.at[:, members * cells - HALO :],
            road_all.at[:, left],
            road_send.at[0],
            road_recv.at[0],
            device(0, slab + 1, blocks),
        )

    def road_left():
        return remote(
            road.at[:, :HALO],
            road_all.at[:, right],
            road_send.at[1],
            road_recv.at[1],
            device(members - 1, slab - 1, blocks),
        )

    def main_copy(r):
        to = lax.rem(me + r, members)
        return remote(
            load.at[:, own(to * cells, cells)],
            state.at[mine, centre],
            main_send.at[r - 1],
            main_recv.at[me],
            device(to, slab, blocks),
        )

    def left_copy(r):
        to = lax.rem(me + r, members)
        return to > 0, remote(
            load.at[:, own(jnp.maximum(to * cells - HALO, 0), HALO)],
            state.at[mine, left],
            left_send.at[r - 1],
            left_recv.at[me],
            device(to, slab, blocks),
        )

    def right_copy(r):
        to = lax.rem(me + r, members)
        return to < members - 1, remote(
            load.at[:, own(jnp.minimum((to + 1) * cells, (members - 1) * cells), HALO)],
            state.at[mine, right],
            right_send.at[r - 1],
            right_recv.at[me],
            device(to, slab, blocks),
        )

    def noise_copy(r):
        to = lax.rem(me + r, members)
        return remote(
            noise.at[:, own(to * slots, slots)],
            noise_all.at[mine, :],
            noise_send.at[r - 1],
            noise_recv.at[me],
            device(to, slab, blocks),
        )

    @pl.when(has_right)
    def _():
        edge_right().start()

    @pl.when(has_left)
    def _():
        edge_left().start()

    @pl.when(has_right & first)
    def _():
        road_right().start()

    @pl.when(has_left & last)
    def _():
        road_left().start()

    for r in range(1, members):
        for needed, copy in (left_copy(r), right_copy(r)):
            pl.when(needed)(copy.start)
    for r in range(1, members):
        main_copy(r).start()
    for r in range(1, members):
        noise_copy(r).start()

    state[mine, centre] = load[:, own(me * cells, cells)]
    noise_all[mine, :] = noise[:, own(me * slots, slots)]
    road_all[:, centre] = road[:, own(me * cells, cells)]

    @pl.when(jnp.logical_not(first))
    def _():
        spot = own(jnp.maximum(me * cells - HALO, 0), HALO)
        state[mine, left] = load[:, spot]
        road_all[:, left] = road[:, spot]

    @pl.when(jnp.logical_not(last))
    def _():
        spot = own(jnp.minimum((me + 1) * cells, (members - 1) * cells), HALO)
        state[mine, right] = load[:, spot]
        road_all[:, right] = road[:, spot]

    @pl.when(first & jnp.logical_not(has_left))
    def _():
        state[:, left] = jnp.zeros((members * rows, HALO), jnp.float32)
        road_all[:, left] = jnp.zeros((8, HALO), jnp.float32)

    @pl.when(last & jnp.logical_not(has_right))
    def _():
        state[:, right] = jnp.zeros((members * rows, HALO), jnp.float32)
        row = lax.broadcasted_iota(jnp.int32, (8, HALO), 0)
        exit_value = road[:, members * cells - 1 :]
        ghost = jnp.where(row == 1, 1.0, jnp.where(row == 2, 1e30, 0.0))
        road_all[:, right] = jnp.where(row == 3, exit_value, ghost)

    def arrive(dst, sem):
        remote(dst, dst, main_send.at[0], sem, device(lax.rem(me + 1, members), slab, blocks)).wait_recv()

    for r in range(1, members):
        origin = lax.rem(me + r, members)
        from_rows = pl.ds(pl.multiple_of(origin * rows, rows), rows)
        arrive(state.at[from_rows, centre], main_recv.at[origin])
        arrive(noise_all.at[from_rows, :], noise_recv.at[origin])

        @pl.when(jnp.logical_not(first))
        def _():
            arrive(state.at[from_rows, left], left_recv.at[origin])

        @pl.when(jnp.logical_not(last))
        def _():
            arrive(state.at[from_rows, right], right_recv.at[origin])

    @pl.when(first & has_left)
    def _():
        for origin in range(members):
            arrive(state.at[pl.ds(origin * rows, rows), left], left_recv.at[origin])
        arrive(road_all.at[:, left], road_recv.at[0])

    @pl.when(last & has_right)
    def _():
        for origin in range(members):
            arrive(state.at[pl.ds(origin * rows, rows), right], right_recv.at[origin])
        arrive(road_all.at[:, right], road_recv.at[1])

    for r in range(1, members):
        main_copy(r).wait_send()
        noise_copy(r).wait_send()
        for needed, copy in (left_copy(r), right_copy(r)):
            pl.when(needed)(copy.wait_send)

    @pl.when(has_right)
    def _():
        edge_right().wait_send()

    @pl.when(has_left)
    def _():
        edge_left().wait_send()

    @pl.when(has_right & first)
    def _():
        road_right().wait_send()

    @pl.when(has_left & last)
    def _():
        road_left().wait_send()


def block_kernel(
    sizes, counts, state, noise, road, cell, value, variance, anomaly, mean, products, parts, roads, forecast
):
    members, regions, blocks = sizes
    me = lax.axis_index("member")
    rows, width = state.shape
    cells = width - 2 * HALO
    slots = noise.shape[1]
    for i in range(4):
        roads[i] = jnp.broadcast_to(road[i : i + 1, :], (8, width))

    step_rows = 32

    def wide(value):
        return jnp.concatenate([value] * (step_rows // 8), axis=0)

    def group(g, total):
        here = pl.ds(pl.multiple_of(g * step_rows, step_rows), step_rows)

        def tick(_, now):
            speed, wave, jam, cap = (wide(roads[i]) for i in range(4))
            demand = jnp.minimum(speed * now, cap)
            supply = jnp.minimum(cap, wave * (jam - now))
            entering = jnp.minimum(pltpu.roll(demand, 1, 1), supply)
            leaving = jnp.minimum(demand, pltpu.roll(supply, width - 1, 1))
            return now + entering - leaving

        done = lax.fori_loop(0, HORIZON_TICKS, tick, state[here, :])
        inner = done[:, HALO : HALO + cells]
        forecast[here, :] = inner
        return total + sum(inner[8 * i : 8 * i + 8] for i in range(step_rows // 8))

    total = lax.fori_loop(0, rows // step_rows, group, jnp.zeros((8, cells), jnp.float32))
    average = jnp.sum(total, axis=0, keepdims=True) / rows
    mean[...] = jnp.broadcast_to(average, mean.shape)

    mine = pl.ds(pl.multiple_of(me * slots, HALO), slots)
    spots = cell[:, mine]
    depth = 256
    picked = jnp.zeros((3 * rows, slots), jnp.float32)
    for c in range(cells // depth):
        part = forecast[:, c * depth : (c + 1) * depth]
        high = part.astype(jnp.bfloat16)
        rest = part - high.astype(jnp.float32)
        middle = rest.astype(jnp.bfloat16)
        low = (rest - middle.astype(jnp.float32)).astype(jnp.bfloat16)
        hot = lax.broadcasted_iota(jnp.int32, (depth, slots), 0) + c * depth == spots
        picked = picked + jnp.dot(
            jnp.concatenate([high, middle, low], axis=0),
            jnp.where(hot, 1.0, 0.0).astype(jnp.bfloat16),
            preferred_element_type=jnp.float32,
        )
        anomaly[:, c * depth : (c + 1) * depth] = part - average[:, c * depth : (c + 1) * depth]
    seen = picked[:rows] + picked[rows : 2 * rows] + picked[2 * rows :]
    obs_mean = jnp.sum(seen, axis=0, keepdims=True) / rows
    departure = seen - obs_mean
    var = variance[:, mine]
    live = (lax.broadcasted_iota(jnp.int32, (1, slots), 1) < counts[me]).astype(jnp.float32)
    weight = live / var
    misfit = value[:, mine] - obs_mean
    spread = jnp.sum(departure * departure, axis=0, keepdims=True) / (rows - 1)
    first = jnp.sum(misfit * misfit * weight, axis=1, keepdims=True)
    second = jnp.sum(live * (spread / var + 1.0), axis=1, keepdims=True)
    row = lax.broadcasted_iota(jnp.int32, parts.shape, 0)
    parts[...] = jnp.where(row == 0, first, jnp.where(row == 1, second, 0.0))
    scaled = departure * weight
    perturbed = misfit + jnp.sqrt(var) * noise[...]
    contract = (((1,), (1,)), ((), ()))
    products[:, :rows] = lax.dot_general(
        scaled, departure, contract, precision=HIGHEST, preferred_element_type=jnp.float32
    )
    products[:, rows:] = lax.dot_general(
        scaled, perturbed, contract, precision=HIGHEST, preferred_element_type=jnp.float32
    )


def neighbour_kernel(
    sizes,
    select,
    products,
    parts,
    total,
    sums,
    slab_in,
    outgoing,
    incoming,
    parts_in,
    parts_sum,
    parts_all,
    slab_send,
    slab_recv,
    plane_send,
    plane_recv,
    part_send,
    part_recv,
    wide_send,
    wide_recv,
):
    members, regions, blocks = sizes
    slabs = regions * blocks
    me, slab = position(regions, blocks)
    has_left, has_right = slab > 0, slab < slabs - 1
    for r in range(1, members):
        greet(device(lax.rem(me + r, members), slab, blocks))
    for r in range(1, slabs):
        greet(device(me, lax.rem(slab + r, slabs), blocks))
    pl.semaphore_wait(pltpu.get_barrier_semaphore(), members + slabs - 2)

    def up():
        return remote(
            products, slab_in.at[0], slab_send.at[0], slab_recv.at[0], device(me, slab + 1, blocks)
        )

    def down():
        return remote(
            products, slab_in.at[1], slab_send.at[1], slab_recv.at[1], device(me, slab - 1, blocks)
        )

    def part_copy(r):
        to = lax.rem(me + r, members)
        return remote(
            parts, parts_in.at[me], part_send.at[r - 1], part_recv.at[me], device(to, slab, blocks)
        )

    def wide_copy(r):
        to = lax.rem(slab + r, slabs)
        return remote(
            parts_sum, parts_all.at[slab], wide_send.at[r - 1], wide_recv.at[slab], device(me, to, blocks)
        )

    def plane_copy(r):
        to = lax.rem(me + r, members)
        return remote(
            outgoing.at[r - 1],
            incoming.at[r - 1],
            plane_send.at[r - 1],
            plane_recv.at[r - 1],
            device(to, slab, blocks),
        )

    for r in range(1, members):
        part_copy(r).start()

    @pl.when(has_right)
    def _():
        up().start()

    @pl.when(has_left)
    def _():
        down().start()

    gathered = parts[...]
    for r in range(1, members):
        origin = lax.rem(me + r, members)
        remote(
            parts, parts_in.at[origin], part_send.at[0], part_recv.at[origin], device(origin, slab, blocks)
        ).wait_recv()
        gathered = gathered + parts_in[origin]
    parts_sum[...] = gathered
    for r in range(1, slabs):
        wide_copy(r).start()

    @pl.when(has_left)
    def _():
        up().wait_recv()

    @pl.when(jnp.logical_not(has_left))
    def _():
        slab_in[0] = jnp.zeros_like(slab_in[0])

    @pl.when(has_right)
    def _():
        down().wait_recv()

    @pl.when(jnp.logical_not(has_right))
    def _():
        slab_in[1] = jnp.zeros_like(slab_in[1])

    def blend(to):
        return (
            select[to * 3] * slab_in[0]
            + select[to * 3 + 1] * products[...]
            + select[to * 3 + 2] * slab_in[1]
        )

    for r in range(1, members):
        outgoing[r - 1] = blend(lax.rem(me + r, members))
        plane_copy(r).start()
    local = blend(me)

    for r in range(1, slabs):
        origin = lax.rem(slab + r, slabs)
        remote(
            parts_sum, parts_all.at[origin], wide_send.at[0], wide_recv.at[origin], device(me, origin, blocks)
        ).wait_recv()
        gathered = gathered + parts_all[origin]
    sums[...] = gathered

    for r in range(1, members):
        plane_copy(r).wait_recv()
        local = local + incoming[r - 1]
    total[...] = local

    for r in range(1, members):
        part_copy(r).wait_send()
        plane_copy(r).wait_send()
    for r in range(1, slabs):
        wide_copy(r).wait_send()

    @pl.when(has_right)
    def _():
        up().wait_send()

    @pl.when(has_left)
    def _():
        down().wait_send()


def dot(a, b):
    return jnp.dot(a, b, precision=HIGHEST, preferred_element_type=jnp.float32)


def invert(block):
    size = block.shape[0]
    row = lax.broadcasted_iota(jnp.int32, (size, size), 0)
    column = lax.broadcasted_iota(jnp.int32, (size, size), 1)
    work = block
    for k in range(size):
        scale = 1.0 / work[k : k + 1, k : k + 1]
        pivot = jnp.where(column[k : k + 1] == k, 1.0, work[k : k + 1, :]) * scale
        factor = work[:, k : k + 1]
        work = jnp.where(
            row == k, pivot, jnp.where(column == k, 0.0, work) - factor * pivot
        )
    return work


def solve_kernel(sizes, total, sums, anomaly, mean, result, work):
    rows = total.shape[0]
    size = 16
    inflation = jnp.sqrt(sums[0:1, 0:1] / sums[1:2, 0:1])
    diagonal = (
        lax.broadcasted_iota(jnp.int32, (rows, rows), 0)
        == lax.broadcasted_iota(jnp.int32, (rows, rows), 1)
    )
    identity = jnp.where(diagonal, float(rows - 1), 0.0)
    work[:, :rows] = identity + inflation * inflation * total[:, :rows]
    work[:, rows:] = identity + inflation * total[:, rows:]
    for p in range(rows // size):
        top, end = p * size, (p + 1) * size
        panel = work[top:end, :]
        update = dot(invert(panel[:, top:end]), panel)
        factor = work[:, top:end]
        work[...] = work[...] - dot(factor, update)
        work[top:end, :] = update
    mixing = inflation * work[:, rows:]
    result[...] = mean[0:1, :] + lax.dot_general(
        mixing,
        anomaly[...],
        (((0,), (0,)), ((), ())),
        precision=HIGHEST,
        preferred_element_type=jnp.float32,
    )


def return_kernel(sizes, result, analysis, send, recv):
    members, regions, blocks = sizes
    me, slab = position(regions, blocks)
    rows = analysis.shape[0]
    cells = result.shape[1]
    for r in range(1, members):
        greet(device(lax.rem(me + r, members), slab, blocks))
    pl.semaphore_wait(pltpu.get_barrier_semaphore(), members - 1)

    def copy(r):
        to = lax.rem(me + r, members)
        return remote(
            result.at[pl.ds(pl.multiple_of(to * rows, rows), rows), :],
            analysis.at[:, pl.ds(pl.multiple_of(me * cells, HALO), cells)],
            send.at[r - 1],
            recv.at[me],
            device(to, slab, blocks),
        )

    for r in range(1, members):
        copy(r).start()
    analysis[:, pl.ds(pl.multiple_of(me * cells, HALO), cells)] = result[
        pl.ds(pl.multiple_of(me * rows, rows), rows), :
    ]
    for r in range(1, members):
        origin = lax.rem(me + r, members)
        spot = analysis.at[:, pl.ds(pl.multiple_of(origin * cells, HALO), cells)]
        remote(spot, spot, send.at[0], recv.at[origin], device(origin, slab, blocks)).wait_recv()
    for r in range(1, members):
        copy(r).wait_send()


def body(
    sizes,
    traffic_load,
    free_speed,
    wave_speed,
    jam_density,
    capacity_share,
    observation_cell,
    obs_count,
    observation_value,
    observation_variance,
    observation_noise,
    block_lists,
):
    members, regions, blocks = sizes
    slabs = regions * blocks
    mem_local, cell_total = traffic_load.shape
    slot_total = observation_cell.shape[0]
    block_total = obs_count.shape[0]
    assert block_total == members
    rows, cells, slots = mem_local * members, cell_total // members, slot_total // members
    f32 = jnp.float32
    dma = pltpu.SemaphoreType.DMA

    capacity = capacity_share * free_speed * wave_speed * jam_density / (free_speed + wave_speed)
    blank = jnp.zeros_like(capacity)
    road = jnp.stack([free_speed, wave_speed, jam_density, capacity, blank, blank, blank, blank])

    state, noise_all, road_all = pl.pallas_call(
        functools.partial(scatter_kernel, sizes),
        out_shape=(
            jax.ShapeDtypeStruct((rows, cells + 2 * HALO), f32),
            jax.ShapeDtypeStruct((rows, slots), f32),
            jax.ShapeDtypeStruct((8, cells + 2 * HALO), f32),
        ),
        in_specs=[VMEM] * 3,
        out_specs=(VMEM,) * 3,
        scratch_shapes=[
            dma((members - 1,)),
            dma((members,)),
            dma((members - 1,)),
            dma((members,)),
            dma((members - 1,)),
            dma((members,)),
            dma((members - 1,)),
            dma((members,)),
            dma((2,)),
            dma((2,)),
            dma((2,)),
        ],
        compiler_params=pltpu.CompilerParams(collective_id=0, has_side_effects=True),
        name="scatter",
    )(traffic_load, observation_noise, road)

    anomaly, mean, products, parts = pl.pallas_call(
        functools.partial(block_kernel, sizes),
        out_shape=(
            jax.ShapeDtypeStruct((rows, cells), f32),
            jax.ShapeDtypeStruct((8, cells), f32),
            jax.ShapeDtypeStruct((rows, 2 * rows), f32),
            jax.ShapeDtypeStruct((8, HALO), f32),
        ),
        in_specs=[SMEM] + [VMEM] * 6,
        out_specs=(VMEM,) * 4,
        scratch_shapes=[
            pltpu.VMEM((4, 8, cells + 2 * HALO), f32),
            pltpu.VMEM((rows, cells), f32),
        ],
        name="block",
    )(
        obs_count,
        state,
        noise_all,
        road_all,
        observation_cell.reshape(1, -1),
        observation_value.reshape(1, -1),
        observation_variance.reshape(1, -1),
    )

    slab = lax.axis_index(("region", "block"))
    named = (slab + jnp.arange(-1, 2, dtype=jnp.int32)) * block_total + lax.axis_index("member")
    select = jnp.sum((block_lists[:, None, :] == named[None, :, None]).astype(f32), axis=2).reshape(-1)

    total, sums = pl.pallas_call(
        functools.partial(neighbour_kernel, sizes),
        out_shape=(
            jax.ShapeDtypeStruct((rows, 2 * rows), f32),
            jax.ShapeDtypeStruct((8, HALO), f32),
        ),
        in_specs=[SMEM, VMEM, VMEM],
        out_specs=(VMEM, VMEM),
        scratch_shapes=[
            pltpu.VMEM((2, rows, 2 * rows), f32),
            pltpu.VMEM((members - 1, rows, 2 * rows), f32),
            pltpu.VMEM((members - 1, rows, 2 * rows), f32),
            pltpu.VMEM((members, 8, HALO), f32),
            pltpu.VMEM((8, HALO), f32),
            pltpu.VMEM((slabs, 8, HALO), f32),
            dma((2,)),
            dma((2,)),
            dma((members - 1,)),
            dma((members - 1,)),
            dma((members - 1,)),
            dma((members,)),
            dma((slabs - 1,)),
            dma((slabs,)),
        ],
        compiler_params=pltpu.CompilerParams(collective_id=1, has_side_effects=True),
        name="neighbours",
    )(select, products, parts)

    result = pl.pallas_call(
        functools.partial(solve_kernel, sizes),
        out_shape=jax.ShapeDtypeStruct((rows, cells), f32),
        in_specs=[VMEM] * 4,
        out_specs=VMEM,
        scratch_shapes=[pltpu.VMEM((rows, 2 * rows), f32)],
        name="solve",
    )(total, sums, anomaly, mean)

    return pl.pallas_call(
        functools.partial(return_kernel, sizes),
        out_shape=jax.ShapeDtypeStruct((mem_local, cell_total), f32),
        in_specs=[VMEM],
        out_specs=VMEM,
        scratch_shapes=[dma((members - 1,)), dma((members,))],
        compiler_params=pltpu.CompilerParams(collective_id=2, has_side_effects=True),
        name="give_back",
    )(result)


def solution(mesh):
    slab = P(("region", "block"))
    placed = (
        P("member", ("region", "block")),
        slab,
        slab,
        slab,
        slab,
        slab,
        slab,
        slab,
        slab,
        P("member", ("region", "block")),
        P(("region", "block"), None),
    )
    sizes = (mesh.shape["member"], mesh.shape["region"], mesh.shape["block"])
    return jax.shard_map(
        functools.partial(body, sizes),
        mesh=mesh,
        in_specs=placed,
        out_specs=P("member", ("region", "block")),
        check_vma=False,
    )
```
